32 devices in a mesh: dp: 4 (over y, x), fsdp: 8 (over z, core).
Axes of the slice: x: 2, y: 2, z: 4, core: 2. Of those that a mesh axis runs over, the one named last changes fastest.
Arguments:
- tokens: bfloat16 [96, 257, 1408], P(('dp', 'fsdp')), parts along dimension 0, may hold values from -16 to 16
- ln1_gain: float32 [1408], replicated, may hold values from 0.1 to 1.9
- ln1_bias: float32 [1408], replicated, may hold values from -3 to 3
- qkv_weight: bfloat16 [1408, 4224], P('fsdp'), may hold values from -3 to 3
- qkv_bias: float32 [4224], replicated, may hold values from -3 to 3
- proj_weight: bfloat16 [1408, 1408], P('fsdp'), may hold values from -0.15625 to 0.15625
- proj_bias: float32 [1408], replicated, may hold values from -3 to 3
- ln2_gain: float32 [1408], replicated, may hold values from 0.1 to 1.9
- ln2_bias: float32 [1408], replicated, may hold values from -3 to 3
- fc1_weight: bfloat16 [1408, 3072], P('fsdp'), may hold values from -0.15625 to 0.15625
- fc1_bias: float32 [3072], replicated, may hold values from -3 to 3
- fc2_weight: bfloat16 [3072, 1408], P('fsdp'), may hold values from -0.109375 to 0.109375
- fc2_bias: float32 [1408], replicated, may hold values from -3 to 3
Outputs:
- layer_out: bfloat16 [96, 257, 1408], P(('dp', 'fsdp')), parts along dimension 0
The draws below stay inside these ranges and needn't reach their ends.
There are 4 independent parts, one for each index of `dp`. The reference program is written for one: setup_inputs(seed, part) draws one part's arguments, and reference() takes and returns one part's arrays. A program takes and returns all parts, laid end to end along the dimension named above; an argument that names none is the same for every part. Nothing has to cross between parts.
All inputs are finite; a program needn't handle non-finite values.
Results may differ from the reference program's by a relative error of at most 0.0045.
Values may be sent and summed in bfloat16 or wider, within the bound.
A program may use at most 448 MiB of HBM per device.

```python
import math
import jax
import jax.numpy as jnp
from jax import lax

D = 1408
HEADS = 16
HEAD_DIM = 88
FF = 3072
SEQ = 257
IMAGES = 24


def draw_tokens(key, part):
    base_key = jax.random.fold_in(key, 11)
    first, second = jax.random.split(base_key, 2)
    values = jax.random.normal(first, (IMAGES, SEQ, D), jnp.float32)
    row_scale = jnp.exp(jax.random.uniform(second, (IMAGES, SEQ, 1), jnp.float32, math.log(0.5), math.log(8.0)))
    values = jnp.clip(values * row_scale, -16.0, 16.0)
    return values.astype(jnp.bfloat16)


def draw_qkv_weight(key, part):
    base_key = jax.random.fold_in(key, 23)
    values = jax.random.normal(base_key, (D, 3 * D), jnp.float32) * D ** (-0.5)
    values = jnp.clip(values, -3.0, 3.0)
    return values.astype(jnp.bfloat16)


def levels(rng, shape, pieces, low, top_value):
    factor_of = 1.0
    for axis_at, parts in pieces:
        steps = jax.random.uniform(jax.random.fold_in(jax.random.fold_in(rng, 6), axis_at), (parts,), jnp.float32, low / len(pieces), top_value / len(pieces))
        factor_of = factor_of * jnp.repeat(jnp.exp(steps), shape[axis_at] // parts).reshape((-1,) + (1,) * (len(shape) - 1 - axis_at))
    return factor_of


def normal_values(key, extent, width, reach, cuts=(), held_as=jnp.bfloat16):
    factor_of = levels(key, extent, cuts, -0.22, 0.18) if cuts else 1.0
    entries = jax.random.normal(key, extent, jnp.float32) * width * factor_of
    return jnp.minimum(jnp.maximum(entries, -reach), reach).astype(held_as)


def setup_inputs(seed: int = 0, part: int = 0) -> dict:
    splits = jax.random.split(jax.random.key(seed), 14)
    own_keys = jax.random.split(jax.random.fold_in(splits[13], part), 14)
    return {
        "tokens": draw_tokens(jax.random.fold_in(jax.random.fold_in(splits[13], part), 71), part),
        "ln1_gain": jnp.clip(1.0 + 0.18 * jax.random.normal(splits[1], (D,), jnp.float32), 0.1, 1.9),
        "ln1_bias": normal_values(splits[2], (D,), 0.5, 3.0, (), jnp.float32),
        "qkv_weight": draw_qkv_weight(jax.random.fold_in(splits[13], 71), part),
        "qkv_bias": normal_values(splits[4], (3 * D,), 0.5, 3.0, (), jnp.float32),
        "proj_weight": normal_values(splits[5], (D, D), D ** -0.5, 0.15625, ((0, 8),)),
        "proj_bias": normal_values(splits[6], (D,), 0.5, 3.0, (), jnp.float32),
        "ln2_gain": jnp.clip(1.0 + 0.18 * jax.random.normal(splits[7], (D,), jnp.float32), 0.1, 1.9),
        "ln2_bias": normal_values(splits[8], (D,), 0.5, 3.0, (), jnp.float32),
        "fc1_weight": normal_values(splits[9], (D, FF), D ** -0.5, 0.15625, ((0, 8),)),
        "fc1_bias": normal_values(splits[10], (FF,), 0.5, 3.0, (), jnp.float32),
        "fc2_weight": normal_values(splits[11], (FF, D), FF ** -0.5, 0.109375, ((0, 8),)),
        "fc2_bias": normal_values(splits[12], (D,), 0.5, 3.0, (), jnp.float32),
    }


def layer_norm(values, gain, bias):
    average = lax.optimization_barrier(jnp.mean(values, axis=-1, keepdims=True))
    centered = values - average
    variance = lax.optimization_barrier(jnp.mean(centered * centered, axis=-1, keepdims=True))
    return centered * lax.rsqrt(variance + 1e-06) * gain + bias

def reference(tokens, ln1_gain, ln1_bias, qkv_weight, qkv_bias, proj_weight, proj_bias, ln2_gain, ln2_bias, fc1_weight, fc1_bias, fc2_weight, fc2_bias):
    flat_rows = tokens.reshape(-1, D).astype(jnp.float32)
    normed = layer_norm(flat_rows, ln1_gain, ln1_bias).astype(jnp.bfloat16)
    qkv_proj = (jnp.dot(normed, qkv_weight, preferred_element_type=jnp.float32) + qkv_bias).astype(jnp.bfloat16)
    qkv_proj = qkv_proj.reshape(IMAGES, SEQ, 3, HEADS, HEAD_DIM)
    score_scale = HEAD_DIM ** (-0.5)

    def attend(image):
        queries = image[:, 0].astype(jnp.float32)
        key_part = image[:, 1].astype(jnp.float32)
        value_part = image[:, 2].astype(jnp.float32)
        scores = jnp.einsum('qhd,khd->hqk', queries, key_part) * score_scale
        probs = jax.nn.softmax(scores, axis=-1).astype(jnp.bfloat16)
        mixed = jnp.einsum('hqk,khd->qhd', probs.astype(jnp.float32), value_part)
        return mixed.astype(jnp.bfloat16).reshape(SEQ, D)
    attended = lax.map(attend, qkv_proj).reshape(-1, D)
    resid = jnp.dot(attended, proj_weight, preferred_element_type=jnp.float32) + proj_bias + flat_rows
    normed_two = layer_norm(resid, ln2_gain, ln2_bias).astype(jnp.bfloat16)
    hidden = jax.nn.gelu(jnp.dot(normed_two, fc1_weight, preferred_element_type=jnp.float32) + fc1_bias, approximate=False).astype(jnp.bfloat16)
    result = jnp.dot(hidden, fc2_weight, preferred_element_type=jnp.float32) + fc2_bias + resid
    return result.astype(jnp.bfloat16).reshape(IMAGES, SEQ, D)
```

```python
import functools
import jax
import jax.numpy as jnp
from jax import lax
from jax.experimental import pallas as pl
from jax.experimental.pallas import tpu as pltpu
from jax.sharding import PartitionSpec as P

HEADS = 16


def layer_norm(values, gain, bias):
    average = jnp.mean(values, axis=-1, keepdims=True)
    centered = values - average
    variance = jnp.mean(centered * centered, axis=-1, keepdims=True)
    return centered * lax.rsqrt(variance + 1e-06) * gain + bias


def gather(block):
    return lax.all_gather(block, "fsdp", axis=0, tiled=True)


def gather_by_share(block):
    shares = lax.axis_size("dp")
    rows, columns = block.shape
    if shares & (shares - 1) or rows % (shares * 8):
        return None
    depth = rows // shares
    me = lax.axis_index("dp")
    share = lax.dynamic_slice_in_dim(block, me * depth, depth, 0)
    return gather(share).reshape(-1, depth, columns)


def exchange(share):
    shares = lax.axis_size("dp")
    me = lax.axis_index("dp")
    pieces = jnp.stack(
        [share]
        + [
            lax.ppermute(share, "dp", [(i, i ^ step) for i in range(shares)])
            for step in range(1, shares)
        ]
    )
    ordered = [
        lax.dynamic_index_in_dim(pieces, jnp.bitwise_xor(me, at), 0, keepdims=False)
        for at in range(shares)
    ]
    return jnp.stack(ordered, axis=1).reshape(-1, share.shape[2])


def after(block, earlier):
    return lax.optimization_barrier((block, earlier))


def product(left, weight):
    return jnp.dot(left, weight, preferred_element_type=jnp.float32)


def attend_kernel(head_size, q_ref, k_ref, v_ref, out_ref):
    scale = head_size ** (-0.5)
    for head in range(q_ref.shape[2] // head_size):
        at = slice(head * head_size, (head + 1) * head_size)
        scores = lax.dot_general(
            q_ref[0, :, at],
            k_ref[0, :, at],
            (((1,), (1,)), ((), ())),
            preferred_element_type=jnp.float32,
        )
        top = jnp.max(scores, axis=-1, keepdims=True)
        weights = jnp.exp((scores - top) * scale)
        probs = weights / jnp.sum(weights, axis=-1, keepdims=True)
        mixed = jnp.dot(
            probs.astype(jnp.bfloat16), v_ref[0, :, at], preferred_element_type=jnp.float32
        )
        out_ref[0, :, at] = mixed.astype(jnp.bfloat16)


def attend(qkv, head_size):
    images, seq_len, wide = qkv.shape
    width = wide // 3
    spec = [
        pl.BlockSpec((1, seq_len, width), functools.partial(lambda part, i: (i, 0, part), part))
        for part in range(3)
    ]
    return pl.pallas_call(
        functools.partial(attend_kernel, head_size),
        grid=(images,),
        in_specs=spec,
        out_specs=pl.BlockSpec((1, seq_len, width), lambda i: (i, 0, 0)),
        out_shape=jax.ShapeDtypeStruct((images, seq_len, width), jnp.bfloat16),
        compiler_params=pltpu.CompilerParams(vmem_limit_bytes=48 * 1024 * 1024),
        cost_estimate=pl.CostEstimate(
            flops=4 * images * seq_len * seq_len * width,
            bytes_accessed=8 * images * seq_len * width,
            transcendentals=images * seq_len * seq_len * width // head_size,
        ),
    )(qkv, qkv, qkv)


def on_device(
    tokens,
    ln1_gain,
    ln1_bias,
    qkv_weight,
    qkv_bias,
    proj_weight,
    proj_bias,
    ln2_gain,
    ln2_bias,
    fc1_weight,
    fc1_bias,
    fc2_weight,
    fc2_bias,
):
    images = tokens.shape[0]
    seq_len = tokens.shape[1]
    width = tokens.shape[2]
    head_count = HEADS
    head_size = width // head_count
    flat_rows = tokens.reshape(-1, width)
    resid_input = flat_rows.astype(jnp.float32)
    normed = layer_norm(resid_input, ln1_gain, ln1_bias).astype(jnp.bfloat16)
    row_count = normed.shape[0]
    fc2_share = gather_by_share(fc2_weight)
    fc1_weight, normed = after(fc1_weight, normed)
    qkv_sum = product(normed, gather(qkv_weight))
    qkv_proj = (qkv_sum + qkv_bias).astype(jnp.bfloat16).reshape(images, seq_len, 3 * width)
    if fc2_share is None:
        fc2_weight, qkv_proj = after(fc2_weight, qkv_proj)
        fc2_full = gather(fc2_weight)
    else:
        fc2_share, qkv_proj = after(fc2_share, qkv_proj)
        fc2_full = exchange(fc2_share)
    attended = attend(qkv_proj, head_size).reshape(row_count, width)
    projected = product(attended, gather(proj_weight))
    resid = projected + proj_bias + resid_input
    normed_two = layer_norm(resid, ln2_gain, ln2_bias).astype(jnp.bfloat16)
    fc2_full, normed_two = after(fc2_full, normed_two)
    pre_act = product(normed_two, gather(fc1_weight))
    hidden = jax.nn.gelu(pre_act + fc1_bias, approximate=False).astype(jnp.bfloat16)
    hidden = lax.optimization_barrier(hidden)
    down = product(hidden, fc2_full)
    result = down + fc2_bias + resid
    return result.astype(jnp.bfloat16).reshape(images, seq_len, width)


def solution(mesh):
    placed = (
        P(("dp", "fsdp"), None, None),
        P(),
        P(),
        P("fsdp", None),
        P(),
        P("fsdp", None),
        P(),
        P(),
        P(),
        P("fsdp", None),
        P(),
        P("fsdp", None),
        P(),
    )
    return jax.shard_map(
        on_device,
        mesh=mesh,
        in_specs=placed,
        out_specs=P(("dp", "fsdp"), None, None),
        check_vma=False,
    )
```
